32 devices in a mesh: hi: 4 (over z), lo: 8 (over y, x, core).
Axes of the slice: x: 2, y: 2, z: 4, core: 2. Of those that a mesh axis runs over, the one named last changes fastest.
Arguments:
- state: float32 [2, 33554432], P(None, ('hi', 'lo')), may hold values from -6 to 6
Outputs:
- transformed: float32 [2, 33554432], P(None, ('hi', 'lo'))
The draws below stay inside these ranges and needn't reach their ends.
All inputs are finite; a program needn't handle non-finite values.
Results may differ from the reference program's by a relative error of at most 0.0003.
Values sent between devices are 32-bit elements.
A program may use at most 128 MiB of HBM per device.

```python
import math
import jax
import jax.numpy as jnp
from jax import lax

AMPS = 33554432


def level_of(own_key, shape, shards, low, high):
    level = 1.0
    for dim, shards_of in shards:
        heights = jax.random.uniform(jax.random.fold_in(jax.random.fold_in(own_key, 6), dim), (shards_of,), jnp.float32, low / len(shards), high / len(shards))
        level = level * jnp.repeat(jnp.exp(heights), shape[dim] // shards_of).reshape((-1,) + (1,) * (len(shape) - 1 - dim))
    return level


def noise(own_key, dims, width, limit, shards=(), dtype=jnp.bfloat16):
    drawn = jax.random.normal(own_key, dims, jnp.float32) * width
    if len(shards) > 0:
        drawn = level_of(own_key, dims, shards, -0.22, 0.18) * drawn
    return jnp.clip(drawn, min=-limit, max=limit).astype(dtype)


def setup_inputs(seed: int = 0) -> dict:
    key_list = jax.random.split(jax.random.key(seed), 2)
    state = noise(key_list[0], (2, AMPS), 1.0, 6.0, ((1, 32),), jnp.float32)
    return {"state": state}


def reference(state):
    amplitude = lax.complex(state[0], state[1])
    count = amplitude.shape[0]
    spectrum = jnp.fft.ifft(amplitude) * math.sqrt(count)
    return jnp.stack([jnp.real(spectrum), jnp.imag(spectrum)]).astype(jnp.float32)
```

```python
import math

import jax
import jax.numpy as jnp
import numpy as np
from jax import lax
from jax.sharding import PartitionSpec as P

LANES = 128


def product(spec, left, right):
    return jnp.einsum(spec, left, right, precision=lax.Precision.HIGH, preferred_element_type=jnp.float32)


def dft_table(length):
    steps = np.arange(length, dtype=np.int64)
    phases = (steps[:, None] * steps[None, :] % length) * (2.0 * math.pi / length)
    cosine, sine = np.cos(phases) / math.sqrt(length), np.sin(phases) / math.sqrt(length)
    table = np.stack([np.stack([cosine, -sine], 1), np.stack([sine, cosine], 1)])
    return table.astype(np.float32)


def unit(indices, length):
    phases = (indices % length).astype(jnp.float32) * (2.0 * math.pi / length)
    return jnp.cos(phases), jnp.sin(phases)


def fixed_unit(left, right, length):
    phases = (np.arange(left)[:, None] * np.arange(right)[None, :] % length) * (2.0 * math.pi / length)
    return np.cos(phases).astype(np.float32), np.sin(phases).astype(np.float32)


def times(left, right):
    return (left[0] * right[0] - left[1] * right[1], left[0] * right[1] + left[1] * right[0])


def swap(blocks):
    return lax.all_to_all(blocks, ("hi", "lo"), split_axis=1, concat_axis=1, tiled=True)


def shards(state):
    count_low = lax.axis_size("lo")
    count = lax.axis_size("hi") * count_low
    me = lax.axis_index("hi") * count_low + lax.axis_index("lo")
    amplitudes = state.shape[1]
    whole = amplitudes * count
    mid = amplitudes // (count * LANES)
    low = count * mid
    blocks = state.reshape(2, mid, count, LANES).transpose(0, 2, 1, 3)
    x = swap(blocks)
    x = product("vkut,utab->vkab", dft_table(count), x)
    rest = me * LANES + jnp.arange(LANES, dtype=jnp.int32)
    rest_re, rest_im = unit(jnp.arange(count, dtype=jnp.int32)[:, None] * rest[None, :], whole)
    own_re, own_im = fixed_unit(count, mid, low)
    turn = times((own_re[:, :, None], own_im[:, :, None]), (rest_re[:, None, :], rest_im[:, None, :]))
    x = jnp.stack(times((x[0], x[1]), turn))
    x = product("vkua,uqab->vkqb", dft_table(mid), x)
    turn = unit(jnp.arange(mid, dtype=jnp.int32)[:, None] * rest[None, :], whole // count)
    x = jnp.stack(times((x[0], x[1]), (turn[0][:, None, :], turn[1][:, None, :])))
    x = swap(x.reshape(2, count, mid, LANES))
    x = product("vkud,udqb->vkqb", dft_table(count), x)
    turn = fixed_unit(count, LANES, count * LANES)
    x = jnp.stack(times((x[0], x[1]), (turn[0][:, None, :], turn[1][:, None, :])))
    x = product("vkub,upqb->vkpq", dft_table(LANES), x)
    x = swap(x.reshape(2, count, LANES // count * count, mid))
    return x.transpose(0, 2, 1, 3).reshape(2, amplitudes)


def solution(mesh):
    placed = (P(None, ("hi", "lo")),)
    return jax.shard_map(
        shards, mesh=mesh, in_specs=placed, out_specs=P(None, ("hi", "lo")), check_vma=False
    )
```

```python
import functools
import math

import jax
import jax.numpy as jnp
import numpy as np
from jax import lax
from jax.experimental import pallas as pl
from jax.experimental.pallas import tpu as pltpu
from jax.sharding import PartitionSpec as P

LANES = 128


def product(spec, left, right):
    return jnp.einsum(spec, left, right, precision=lax.Precision.HIGH, preferred_element_type=jnp.float32)


def dft_table(length):
    steps = np.arange(length, dtype=np.int64)
    phases = (steps[:, None] * steps[None, :] % length) * (2.0 * math.pi / length)
    cosine, sine = np.cos(phases) / math.sqrt(length), np.sin(phases) / math.sqrt(length)
    table = np.stack([np.stack([cosine, -sine], 1), np.stack([sine, cosine], 1)])
    return table.astype(np.float32)


def unit(indices, length):
    phases = (indices % length).astype(jnp.float32) * (2.0 * math.pi / length)
    return jnp.cos(phases), jnp.sin(phases)


def fixed_unit(left, right, length):
    phases = (np.arange(left)[:, None] * np.arange(right)[None, :] % length) * (2.0 * math.pi / length)
    return np.cos(phases).astype(np.float32), np.sin(phases).astype(np.float32)


def times(left, right):
    return (left[0] * right[0] - left[1] * right[1], left[0] * right[1] + left[1] * right[0])


def swap(blocks):
    return lax.all_to_all(blocks, ("hi", "lo"), split_axis=1, concat_axis=1, tiled=True)


def halves(value):
    high = value.astype(jnp.bfloat16)
    return high, (value - high.astype(jnp.float32)).astype(jnp.bfloat16)


def table_halves(length):
    table = dft_table(length).reshape(2 * length, 2 * length)
    high = table.astype(jnp.bfloat16)
    low = (table - high.astype(np.float32)).astype(jnp.bfloat16)
    return np.concatenate([high, high, low], axis=1)


def mix(table, data):
    high, low = halves(data)
    parts = jnp.concatenate([high, low, high], axis=0)
    return jnp.dot(table, parts, preferred_element_type=jnp.float32)


def call(kernel, shape, *operands, scratch=()):
    return pl.pallas_call(
        kernel,
        out_shape=jax.ShapeDtypeStruct(shape, jnp.float32),
        scratch_shapes=[pltpu.VMEM(s, jnp.float32) for s in scratch],
        compiler_params=pltpu.CompilerParams(vmem_limit_bytes=60 * 2**20),
    )(*operands)


def entry_kernel(count, mid, x_ref, o_ref):
    @pl.loop(0, count)
    def _(d):
        for u in range(2):
            o_ref[pl.ds((u * count + d) * mid, mid), :] = x_ref[pl.ds(d * 2 + u, mid, stride=2 * count), :]


def first_kernel(count, mid, x_ref, t1_ref, t2_ref, own_ref, rest_ref, turn_ref, z_ref, y_ref):
    low = count * mid

    @pl.loop(0, mid // 8)
    def _(c):
        cols = []
        for i in range(8):
            cols.append(jnp.concatenate([x_ref[pl.ds(u * low + c * 8 + i, count, stride=mid), :] for u in range(2)], axis=0))
        out = mix(t1_ref[...], jnp.concatenate(cols, axis=1))
        rest = (rest_ref[0], rest_ref[1])
        for i in range(8):
            own = (own_ref[0, c, :, i : i + 1], own_ref[1, c, :, i : i + 1])
            mine = out[:, i * LANES : (i + 1) * LANES]
            got = times(times((mine[:count], mine[count:]), own), rest)
            for u in range(2):
                y_ref[pl.ds(u * low + c * 8 + i, count, stride=mid), :] = got[u]

    @pl.loop(0, count // 2)
    def _(c):
        cols = []
        for i in range(2):
            cols.append(jnp.concatenate([y_ref[pl.ds(u * low + (c * 2 + i) * mid, mid), :] for u in range(2)], axis=0))
        out = mix(t2_ref[...], jnp.concatenate(cols, axis=1))
        turn = (turn_ref[0], turn_ref[1])
        for i in range(2):
            mine = out[:, i * LANES : (i + 1) * LANES]
            got = times((mine[:mid], mine[mid:]), turn)
            for u in range(2):
                z_ref[pl.ds(u * low + c * 2 + i, mid, stride=count), :] = got[u]


def second_kernel(count, mid, x_ref, t3_ref, t4_ref, turn_ref, o_ref, s_ref):
    low = count * mid
    pages = mid // LANES

    @pl.loop(0, mid // 8)
    def _(c):
        cols = []
        for i in range(8):
            cols.append(jnp.concatenate([x_ref[pl.ds(u * low + c * 8 + i, count, stride=mid), :] for u in range(2)], axis=0))
        out = mix(t3_ref[...], jnp.concatenate(cols, axis=1))
        turn = (turn_ref[0], turn_ref[1])
        for i in range(8):
            mine = out[:, i * LANES : (i + 1) * LANES]
            got = times((mine[:count], mine[count:]), turn)
            for u in range(2):
                s_ref[pl.ds(u * low + c * 8 + i, count, stride=mid), :] = got[u]

    @pl.loop(0, count)
    def _(k2):
        high, lows = halves(jnp.concatenate([s_ref[pl.ds(u * low + k2 * mid, mid), :] for u in range(2)], axis=1))
        parts = jnp.concatenate([high, lows, high], axis=1)
        out = lax.dot_general(t4_ref[...], parts, (((1,), (1,)), ((), ())), preferred_element_type=jnp.float32)
        for v in range(2):
            for h in range(pages):
                o_ref[pl.ds(v * LANES * count * pages + k2 * pages + h, LANES, stride=count * pages), :] = out[
                    v * LANES : (v + 1) * LANES, h * LANES : (h + 1) * LANES
                ]


def final_kernel(count, mid, x_ref, o_ref):
    pages = mid // LANES

    @pl.loop(0, count)
    def _(s):
        for v in range(2):
            for h in range(pages):
                o_ref[pl.ds((s * pages + h) * 2 + v, LANES, stride=count * pages * 2), :] = x_ref[
                    pl.ds((v * count + s) * LANES * pages + h, LANES, stride=pages), :
                ]


def shards_by_kernels(state, count, me):
    amplitudes = state.shape[1]
    whole = amplitudes * count
    mid = amplitudes // (count * LANES)
    low = count * mid
    rows = (2 * low, LANES)
    bind = functools.partial
    x = state.reshape(2, low, LANES).transpose(1, 0, 2).reshape(rows)
    x = call(bind(entry_kernel, count, mid), rows, x)
    x = swap(x.reshape(2, count, mid, LANES)).reshape(rows)
    places = me * LANES + jnp.arange(LANES, dtype=jnp.int32)
    rest = jnp.stack(unit(jnp.arange(count, dtype=jnp.int32)[:, None] * places[None, :], whole))
    turn = jnp.stack(unit(jnp.arange(mid, dtype=jnp.int32)[:, None] * places[None, :], whole // count))
    own = jnp.asarray(np.stack(fixed_unit(count, mid, low)))
    own = own.reshape(2, count, mid // 8, 8).transpose(0, 2, 1, 3)
    x = call(
        bind(first_kernel, count, mid), rows, x, table_halves(count), table_halves(mid), own, rest, turn, scratch=(rows,)
    )
    x = swap(x.reshape(2, count, mid, LANES)).reshape(rows)
    turn = jnp.asarray(np.stack(fixed_unit(count, LANES, count * LANES)))
    x = call(
        bind(second_kernel, count, mid), rows, x, table_halves(count), table_halves(LANES), turn, scratch=(rows,)
    )
    x = swap(x.reshape(2, count, mid, LANES)).reshape(rows)
    x = call(bind(final_kernel, count, mid), rows, x)
    return x.reshape(low, 2, LANES).transpose(1, 0, 2).reshape(2, amplitudes)


def shards(state):
    count_low = lax.axis_size("lo")
    count = lax.axis_size("hi") * count_low
    me = lax.axis_index("hi") * count_low + lax.axis_index("lo")
    amplitudes = state.shape[1]
    whole = amplitudes * count
    mid = amplitudes // (count * LANES)
    low = count * mid
    if mid % LANES == 0 and LANES % count == 0 and count % 8 == 0:
        return shards_by_kernels(state, count, me)
    blocks = state.reshape(2, mid, count, LANES).transpose(0, 2, 1, 3)
    x = swap(blocks)
    x = product("vkut,utab->vkab", dft_table(count), x)
    rest = me * LANES + jnp.arange(LANES, dtype=jnp.int32)
    rest_re, rest_im = unit(jnp.arange(count, dtype=jnp.int32)[:, None] * rest[None, :], whole)
    own_re, own_im = fixed_unit(count, mid, low)
    turn = times((own_re[:, :, None], own_im[:, :, None]), (rest_re[:, None, :], rest_im[:, None, :]))
    x = jnp.stack(times((x[0], x[1]), turn))
    x = product("vkua,uqab->vkqb", dft_table(mid), x)
    turn = unit(jnp.arange(mid, dtype=jnp.int32)[:, None] * rest[None, :], whole // count)
    x = jnp.stack(times((x[0], x[1]), (turn[0][:, None, :], turn[1][:, None, :])))
    x = swap(x.reshape(2, count, mid, LANES))
    x = product("vkud,udqb->vkqb", dft_table(count), x)
    turn = fixed_unit(count, LANES, count * LANES)
    x = jnp.stack(times((x[0], x[1]), (turn[0][:, None, :], turn[1][:, None, :])))
    x = product("vkub,upqb->vkpq", dft_table(LANES), x)
    x = swap(x.reshape(2, count, LANES // count * count, mid))
    return x.transpose(0, 2, 1, 3).reshape(2, amplitudes)


def solution(mesh):
    placed = (P(None, ("hi", "lo")),)
    return jax.shard_map(
        shards, mesh=mesh, in_specs=placed, out_specs=P(None, ("hi", "lo")), check_vma=False
    )
```

```python
import functools
import math

import jax
import jax.numpy as jnp
import numpy as np
from jax import lax
from jax.experimental import pallas as pl
from jax.experimental.pallas import tpu as pltpu
from jax.sharding import PartitionSpec as P

LANES = 128


def product(spec, left, right):
    return jnp.einsum(spec, left, right, precision=lax.Precision.HIGH, preferred_element_type=jnp.float32)


def dft_table(length):
    steps = np.arange(length, dtype=np.int64)
    phases = (steps[:, None] * steps[None, :] % length) * (2.0 * math.pi / length)
    cosine, sine = np.cos(phases) / math.sqrt(length), np.sin(phases) / math.sqrt(length)
    table = np.stack([np.stack([cosine, -sine], 1), np.stack([sine, cosine], 1)])
    return table.astype(np.float32)


def unit(indices, length):
    phases = (indices % length).astype(jnp.float32) * (2.0 * math.pi / length)
    return jnp.cos(phases), jnp.sin(phases)


def fixed_unit(left, right, length):
    phases = (np.arange(left)[:, None] * np.arange(right)[None, :] % length) * (2.0 * math.pi / length)
    return np.cos(phases).astype(np.float32), np.sin(phases).astype(np.float32)


def times(left, right):
    return (left[0] * right[0] - left[1] * right[1], left[0] * right[1] + left[1] * right[0])


def swap(blocks, axis=1):
    return lax.all_to_all(blocks, ("hi", "lo"), split_axis=axis, concat_axis=axis, tiled=True)


def halves(value):
    high = value.astype(jnp.bfloat16)
    return high, (value - high.astype(jnp.float32)).astype(jnp.bfloat16)


def table_halves(length):
    table = dft_table(length).reshape(2 * length, 2 * length)
    high = table.astype(jnp.bfloat16)
    low = (table - high.astype(np.float32)).astype(jnp.bfloat16)
    return np.concatenate([high, high, low], axis=1)


def mix(table, data):
    high, low = halves(data)
    parts = jnp.concatenate([high, low, high], axis=0)
    return jnp.dot(table, parts, preferred_element_type=jnp.float32)


def call(kernel, shape, *operands, scratch=()):
    return pl.pallas_call(
        kernel,
        out_shape=jax.ShapeDtypeStruct(shape, jnp.float32),
        scratch_shapes=[pltpu.VMEM(s, jnp.float32) for s in scratch],
        compiler_params=pltpu.CompilerParams(vmem_limit_bytes=60 * 2**20),
    )(*operands)


STEPS = 4


def entry_kernel(count, x_ref, o_ref):
    @pl.loop(0, count, unroll=2)
    def _(d):
        for u in range(2):
            o_ref[d * 2 + u] = x_ref[pl.ds(d * 2 + u, o_ref.shape[1], stride=2 * count), :]


def first_kernel(count, mid, x_ref, t1_ref, t2_ref, own_ref, rest_ref, turn_ref, z_ref, y_ref):
    low = count * mid
    run = mid // count

    @pl.loop(0, mid // 8, unroll=2)
    def _(c):
        cols = []
        for i in range(8):
            cols.append(jnp.concatenate([x_ref[pl.ds(u * mid + c * 8 + i, count, stride=2 * mid), :] for u in range(2)], axis=0))
        out = mix(t1_ref[...], jnp.concatenate(cols, axis=1))
        rest = (rest_ref[0], rest_ref[1])
        for i in range(8):
            own = (own_ref[0, c, :, i : i + 1], own_ref[1, c, :, i : i + 1])
            mine = out[:, i * LANES : (i + 1) * LANES]
            got = times(times((mine[:count], mine[count:]), own), rest)
            for u in range(2):
                y_ref[pl.ds(u * low + c * 8 + i, count, stride=mid), :] = got[u]

    @pl.loop(0, count // 2, unroll=2)
    def _(c):
        cols = []
        for i in range(2):
            cols.append(jnp.concatenate([y_ref[pl.ds(u * low + (c * 2 + i) * mid, mid), :] for u in range(2)], axis=0))
        out = mix(t2_ref[...], jnp.concatenate(cols, axis=1))
        turn = (turn_ref[0], turn_ref[1])
        for i in range(2):
            mine = out[:, i * LANES : (i + 1) * LANES]
            got = times((mine[:mid], mine[mid:]), turn)
            for d in range(count):
                for u in range(2):
                    z_ref[pl.ds((d * 2 + u) * mid + (c * 2 + i) * run, run), :] = got[u][d * run : (d + 1) * run]


def second_kernel(count, mid, x_ref, t3_ref, t4_ref, turn_ref, o_ref, s_ref):
    low = count * mid
    pages = mid // LANES
    run = mid // count
    tops = LANES // count

    @pl.loop(0, count, unroll=2)
    def _(c):
        cols = []
        for i in range(run):
            cols.append(jnp.concatenate([x_ref[pl.ds(u * mid + c * run + i, count, stride=2 * mid), :] for u in range(2)], axis=0))
        out = mix(t3_ref[...], jnp.concatenate(cols, axis=1))
        turn = (turn_ref[0], turn_ref[1])
        for i in range(run):
            mine = out[:, i * LANES : (i + 1) * LANES]
            got = times((mine[:count], mine[count:]), turn)
            for u in range(2):
                s_ref[pl.ds(u * low + i * count + c, count, stride=mid), :] = got[u]

    @pl.loop(0, count, unroll=2)
    def _(k2):
        high, lows = halves(jnp.concatenate([s_ref[pl.ds(u * low + k2 * mid, mid), :] for u in range(2)], axis=1))
        parts = jnp.concatenate([high, lows, high], axis=1)
        out = lax.dot_general(t4_ref[...], parts, (((1,), (1,)), ((), ())), preferred_element_type=jnp.float32)
        for top in range(tops):
            for v in range(2):
                start = (v * tops + top) * count * pages
                for h in range(pages):
                    o_ref[pl.ds(start + k2 * pages + h, count, stride=2 * mid), :] = out[
                        (top * 2 + v) * count : (top * 2 + v + 1) * count, h * LANES : (h + 1) * LANES
                    ]


def final_kernel(count, mid, x_ref, o_ref):
    pages = mid // LANES
    part = x_ref.shape[1] // pages

    @pl.loop(0, count, unroll=2)
    def _(s):
        for v in range(2):
            for h in range(pages):
                o_ref[pl.ds((s * pages + h) * 2 + v, part, stride=count * pages * 2), :] = x_ref[
                    s * 2 + v, pl.ds(h, part, stride=pages), :
                ]


def shards_by_kernels(state, count, me):
    amplitudes = state.shape[1]
    whole = amplitudes * count
    mid = amplitudes // (count * LANES)
    low = count * mid
    rows = (2 * low, LANES)
    blocks = (2 * count, mid, LANES)
    flat_spec = pl.BlockSpec((2 * low // STEPS, LANES), lambda g: (g, 0))
    block_spec = pl.BlockSpec((2 * count, mid // STEPS, LANES), lambda g: (0, g, 0))
    bind = functools.partial
    x = state.reshape(2, low, LANES).transpose(1, 0, 2).reshape(rows)
    x = pl.pallas_call(
        bind(entry_kernel, count), out_shape=jax.ShapeDtypeStruct(blocks, jnp.float32),
        grid=(STEPS,), in_specs=[flat_spec], out_specs=block_spec,
    )(x)
    x = swap(x.reshape(count, 2 * mid, LANES), 0).reshape(rows)
    places = me * LANES + jnp.arange(LANES, dtype=jnp.int32)
    rest = jnp.stack(unit(jnp.arange(count, dtype=jnp.int32)[:, None] * places[None, :], whole))
    turn = jnp.stack(unit(jnp.arange(mid, dtype=jnp.int32)[:, None] * places[None, :], whole // count))
    own = jnp.asarray(np.stack(fixed_unit(count, mid, low)))
    own = own.reshape(2, count, mid // 8, 8).transpose(0, 2, 1, 3)
    x = call(
        bind(first_kernel, count, mid), rows, x, table_halves(count), table_halves(mid), own, rest, turn, scratch=(rows,)
    )
    x = swap(x.reshape(count, 2 * mid, LANES), 0).reshape(rows)
    turn = jnp.asarray(np.stack(fixed_unit(count, LANES, count * LANES)))
    t4 = table_halves(LANES)
    t4 = t4.reshape(2, count, LANES // count, -1).transpose(2, 0, 1, 3).reshape(t4.shape)
    x = call(bind(second_kernel, count, mid), rows, x, table_halves(count), t4, turn, scratch=(rows,))
    x = swap(x.reshape(count, 2 * mid, LANES), 0).reshape(blocks)
    x = pl.pallas_call(
        bind(final_kernel, count, mid), out_shape=jax.ShapeDtypeStruct(rows, jnp.float32),
        grid=(STEPS,), in_specs=[block_spec], out_specs=flat_spec,
    )(x)
    return x.reshape(low, 2, LANES).transpose(1, 0, 2).reshape(2, amplitudes)


def shards(state):
    count_low = lax.axis_size("lo")
    count = lax.axis_size("hi") * count_low
    me = lax.axis_index("hi") * count_low + lax.axis_index("lo")
    amplitudes = state.shape[1]
    whole = amplitudes * count
    mid = amplitudes // (count * LANES)
    low = count * mid
    if mid % LANES == 0 and LANES % count == 0 and count % 8 == 0 and mid % (8 * count) == 0:
        return shards_by_kernels(state, count, me)
    blocks = state.reshape(2, mid, count, LANES).transpose(0, 2, 1, 3)
    x = swap(blocks)
    x = product("vkut,utab->vkab", dft_table(count), x)
    rest = me * LANES + jnp.arange(LANES, dtype=jnp.int32)
    rest_re, rest_im = unit(jnp.arange(count, dtype=jnp.int32)[:, None] * rest[None, :], whole)
    own_re, own_im = fixed_unit(count, mid, low)
    turn = times((own_re[:, :, None], own_im[:, :, None]), (rest_re[:, None, :], rest_im[:, None, :]))
    x = jnp.stack(times((x[0], x[1]), turn))
    x = product("vkua,uqab->vkqb", dft_table(mid), x)
    turn = unit(jnp.arange(mid, dtype=jnp.int32)[:, None] * rest[None, :], whole // count)
    x = jnp.stack(times((x[0], x[1]), (turn[0][:, None, :], turn[1][:, None, :])))
    x = swap(x.reshape(2, count, mid, LANES))
    x = product("vkud,udqb->vkqb", dft_table(count), x)
    turn = fixed_unit(count, LANES, count * LANES)
    x = jnp.stack(times((x[0], x[1]), (turn[0][:, None, :], turn[1][:, None, :])))
    x = product("vkub,upqb->vkpq", dft_table(LANES), x)
    x = swap(x.reshape(2, count, LANES // count * count, mid))
    return x.transpose(0, 2, 1, 3).reshape(2, amplitudes)


def solution(mesh):
    placed = (P(None, ("hi", "lo")),)
    return jax.shard_map(
        shards, mesh=mesh, in_specs=placed, out_specs=P(None, ("hi", "lo")), check_vma=False
    )
```

```python
import functools
import math

import jax
import jax.numpy as jnp
import numpy as np
from jax import lax
from jax.experimental import pallas as pl
from jax.experimental.pallas import tpu as pltpu
from jax.sharding import PartitionSpec as P

LANES = 128


def product(spec, left, right):
    return jnp.einsum(spec, left, right, precision=lax.Precision.HIGH, preferred_element_type=jnp.float32)


def dft_table(length):
    steps = np.arange(length, dtype=np.int64)
    phases = (steps[:, None] * steps[None, :] % length) * (2.0 * math.pi / length)
    cosine, sine = np.cos(phases) / math.sqrt(length), np.sin(phases) / math.sqrt(length)
    table = np.stack([np.stack([cosine, -sine], 1), np.stack([sine, cosine], 1)])
    return table.astype(np.float32)


def unit(indices, length):
    phases = (indices % length).astype(jnp.float32) * (2.0 * math.pi / length)
    return jnp.cos(phases), jnp.sin(phases)


def fixed_unit(left, right, length):
    phases = (np.arange(left)[:, None] * np.arange(right)[None, :] % length) * (2.0 * math.pi / length)
    return np.cos(phases).astype(np.float32), np.sin(phases).astype(np.float32)


def times(left, right):
    return (left[0] * right[0] - left[1] * right[1], left[0] * right[1] + left[1] * right[0])


def swap(blocks, axis=1):
    return lax.all_to_all(blocks, ("hi", "lo"), split_axis=axis, concat_axis=axis, tiled=True)


def halves(value):
    high = value.astype(jnp.bfloat16)
    return high, (value - high.astype(jnp.float32)).astype(jnp.bfloat16)


def table_halves(length):
    table = dft_table(length).reshape(2 * length, 2 * length)
    high = table.astype(jnp.bfloat16)
    low = (table - high.astype(np.float32)).astype(jnp.bfloat16)
    return np.concatenate([high, high, low], axis=1)


def mix(table, data):
    high, low = halves(data)
    parts = jnp.concatenate([high, low, high], axis=0)
    return jnp.dot(table, parts, preferred_element_type=jnp.float32)


def call(kernel, shape, *operands, scratch=()):
    return pl.pallas_call(
        kernel,
        out_shape=[jax.ShapeDtypeStruct(one, jnp.float32) for one in shape],
        scratch_shapes=[pltpu.VMEM(s, jnp.float32) for s in scratch],
        cost_estimate=pl.CostEstimate(flops=8 * 10**9, bytes_accessed=2**24, transcendentals=0),
        compiler_params=pltpu.CompilerParams(vmem_limit_bytes=60 * 2**20),
    )(*operands)


STEPS = 4


def entry_kernel(count, x_ref, o_ref):
    @pl.loop(0, count, unroll=2)
    def _(d):
        for u in range(2):
            o_ref[d * 2 + u] = x_ref[pl.ds(d * 2 + u, o_ref.shape[1], stride=2 * count), :]


def first_kernel(count, mid, x_ref, t1_ref, t2_ref, own_ref, rest_ref, turn_ref, y_ref, z_ref):
    low = count * mid

    @pl.loop(0, mid // 8, unroll=2)
    def _(c):
        cols = []
        for i in range(8):
            cols.append(jnp.concatenate([x_ref[pl.ds(u * mid + c * 8 + i, count, stride=2 * mid), :] for u in range(2)], axis=0))
        out = mix(t1_ref[...], jnp.concatenate(cols, axis=1))
        rest = (rest_ref[0], rest_ref[1])
        for i in range(8):
            own = (own_ref[0, c, :, i : i + 1], own_ref[1, c, :, i : i + 1])
            mine = out[:, i * LANES : (i + 1) * LANES]
            got = times(times((mine[:count], mine[count:]), own), rest)
            for u in range(2):
                y_ref[pl.ds(u * low + c * 8 + i, count, stride=mid), :] = got[u]

    page_kernel(count, mid, y_ref, t2_ref, turn_ref, z_ref)


def page_kernel(count, mid, y_ref, t2_ref, turn_ref, z_ref):
    low = count * mid
    half = mid // 2
    run = half // count

    @pl.loop(0, count // 2, unroll=2)
    def _(c):
        cols = []
        for i in range(2):
            cols.append(jnp.concatenate([y_ref[pl.ds(u * low + (c * 2 + i) * mid, mid), :] for u in range(2)], axis=0))
        out = mix(t2_ref[...], jnp.concatenate(cols, axis=1))
        turn = (turn_ref[0], turn_ref[1])
        got = []
        for i in range(2):
            mine = out[:, i * LANES : (i + 1) * LANES]
            got.append(times((mine[:half], mine[half:]), turn))
        for d in range(count):
            for u in range(2):
                z_ref[pl.ds((d * 2 + u) * half + c * 2 * run, 2 * run), :] = jnp.concatenate(
                    [got[i][u][d * run : (d + 1) * run] for i in range(2)], axis=0
                )


def second_kernel(count, mid, x_ref, t3_ref, t4_ref, turn_ref, o_ref, s_ref):
    low = count * mid
    pages = mid // LANES
    run = mid // count
    tops = LANES // count

    @pl.loop(0, count, unroll=2)
    def _(c):
        cols = []
        for i in range(run):
            cols.append(jnp.concatenate([x_ref[pl.ds(u * mid + c * run + i, count, stride=2 * mid), :] for u in range(2)], axis=0))
        out = mix(t3_ref[...], jnp.concatenate(cols, axis=1))
        turn = (turn_ref[0], turn_ref[1])
        for i in range(run):
            mine = out[:, i * LANES : (i + 1) * LANES]
            got = times((mine[:count], mine[count:]), turn)
            for u in range(2):
                s_ref[pl.ds(u * low + i * count + c, count, stride=mid), :] = got[u]

    @pl.loop(0, count, unroll=2)
    def _(k2):
        high, lows = halves(jnp.concatenate([s_ref[pl.ds(u * low + k2 * mid, mid), :] for u in range(2)], axis=1))
        parts = jnp.concatenate([high, lows, high], axis=1)
        out = lax.dot_general(t4_ref[...], parts, (((1,), (1,)), ((), ())), preferred_element_type=jnp.float32)
        for top in range(tops):
            for v in range(2):
                start = (v * tops + top) * count * pages
                for h in range(pages):
                    o_ref[pl.ds(start + k2 * pages + h, count, stride=2 * mid), :] = out[
                        (top * 2 + v) * count : (top * 2 + v + 1) * count, h * LANES : (h + 1) * LANES
                    ]


def final_kernel(count, x0_ref, x1_ref, o_ref):
    part = x0_ref.shape[1]

    @pl.loop(0, count, unroll=2)
    def _(s):
        for v in range(2):
            for h, x_ref in enumerate((x0_ref, x1_ref)):
                o_ref[pl.ds((s * 2 + h) * 2 + v, part, stride=count * 4), :] = x_ref[s * 2 + v]


def shards_by_kernels(state, count, me):
    amplitudes = state.shape[1]
    whole = amplitudes * count
    mid = amplitudes // (count * LANES)
    low = count * mid
    rows = (2 * low, LANES)
    blocks = (2 * count, mid, LANES)
    flat_spec = pl.BlockSpec((2 * low // STEPS, LANES), lambda g: (g, 0))
    block_spec = pl.BlockSpec((2 * count, mid // STEPS, LANES), lambda g: (0, g, 0))
    bind = functools.partial
    x = state.reshape(2, low, LANES).transpose(1, 0, 2).reshape(rows)
    x = pl.pallas_call(
        bind(entry_kernel, count), out_shape=jax.ShapeDtypeStruct(blocks, jnp.float32),
        grid=(STEPS,), in_specs=[flat_spec], out_specs=block_spec,
    )(x)
    x = swap(x.reshape(count, 2 * mid, LANES), 0).reshape(rows)
    places = me * LANES + jnp.arange(LANES, dtype=jnp.int32)
    rest = jnp.stack(unit(jnp.arange(count, dtype=jnp.int32)[:, None] * places[None, :], whole))
    turn = jnp.stack(unit(jnp.arange(mid, dtype=jnp.int32)[:, None] * places[None, :], whole // count))
    own = jnp.asarray(np.stack(fixed_unit(count, mid, low)))
    own = own.reshape(2, count, mid // 8, 8).transpose(0, 2, 1, 3)
    half = mid // 2
    pages = (count, 2 * half, LANES)
    flat = (2 * count * half, LANES)
    t2 = table_halves(mid).reshape(2, count, 2, half // count, -1)
    t2 = [t2[:, :, h].reshape(2 * half, -1) for h in range(2)]
    turn = turn.reshape(2, count, 2, half // count, LANES)
    turn = [turn[:, :, h].reshape(2, half, LANES) for h in range(2)]
    y, z0 = call(bind(first_kernel, count, mid), (rows, flat), x, table_halves(count), t2[0], own, rest, turn[0])
    z0 = swap(z0.reshape(pages), 0).reshape(flat)
    (z1,) = call(bind(page_kernel, count, mid), (flat,), y, t2[1], turn[1])
    z1 = swap(z1.reshape(pages), 0).reshape(flat)
    turn = jnp.asarray(np.stack(fixed_unit(count, LANES, count * LANES)))
    t4 = table_halves(LANES)
    t4 = t4.reshape(2, count, LANES // count, -1).transpose(2, 0, 1, 3).reshape(t4.shape)
    done = []
    for z in (z0, z1):
        (z,) = call(bind(second_kernel, count, half), (flat,), z, table_halves(count), t4, turn, scratch=(flat,))
        done.append(swap(z.reshape(pages), 0).reshape(2 * count, half, LANES))
    page_spec = pl.BlockSpec((2 * count, half // STEPS, LANES), lambda g: (0, g, 0))
    x = pl.pallas_call(
        bind(final_kernel, count), out_shape=jax.ShapeDtypeStruct(rows, jnp.float32),
        grid=(STEPS,), in_specs=[page_spec, page_spec], out_specs=flat_spec,
    )(*done)
    return x.reshape(low, 2, LANES).transpose(1, 0, 2).reshape(2, amplitudes)


def shards(state):
    count_low = lax.axis_size("lo")
    count = lax.axis_size("hi") * count_low
    me = lax.axis_index("hi") * count_low + lax.axis_index("lo")
    amplitudes = state.shape[1]
    whole = amplitudes * count
    mid = amplitudes // (count * LANES)
    low = count * mid
    if mid == 2 * LANES and LANES % count == 0 and count % 8 == 0 and mid % (8 * count) == 0:
        return shards_by_kernels(state, count, me)
    blocks = state.reshape(2, mid, count, LANES).transpose(0, 2, 1, 3)
    x = swap(blocks)
    x = product("vkut,utab->vkab", dft_table(count), x)
    rest = me * LANES + jnp.arange(LANES, dtype=jnp.int32)
    rest_re, rest_im = unit(jnp.arange(count, dtype=jnp.int32)[:, None] * rest[None, :], whole)
    own_re, own_im = fixed_unit(count, mid, low)
    turn = times((own_re[:, :, None], own_im[:, :, None]), (rest_re[:, None, :], rest_im[:, None, :]))
    x = jnp.stack(times((x[0], x[1]), turn))
    x = product("vkua,uqab->vkqb", dft_table(mid), x)
    turn = unit(jnp.arange(mid, dtype=jnp.int32)[:, None] * rest[None, :], whole // count)
    x = jnp.stack(times((x[0], x[1]), (turn[0][:, None, :], turn[1][:, None, :])))
    x = swap(x.reshape(2, count, mid, LANES))
    x = product("vkud,udqb->vkqb", dft_table(count), x)
    turn = fixed_unit(count, LANES, count * LANES)
    x = jnp.stack(times((x[0], x[1]), (turn[0][:, None, :], turn[1][:, None, :])))
    x = product("vkub,upqb->vkpq", dft_table(LANES), x)
    x = swap(x.reshape(2, count, LANES // count * count, mid))
    return x.transpose(0, 2, 1, 3).reshape(2, amplitudes)


def solution(mesh):
    placed = (P(None, ("hi", "lo")),)
    return jax.shard_map(
        shards, mesh=mesh, in_specs=placed, out_specs=P(None, ("hi", "lo")), check_vma=False
    )
```
